32 devices in a mesh: row: 4 (over z), col: 4 (over x, core), mp: 2 (over y).
Axes of the slice: x: 2, y: 2, z: 4, core: 2. Of those that a mesh axis runs over, the one named last changes fastest.
Arguments:
- weights: bfloat16 [4, 4, 5, 2304, 1024], P('row', 'col', None, None, 'mp'), may hold values from -6 to 6
- warm_down: bfloat16 [4, 4, 5, 4, 1024], P('row', 'col', None, None, 'mp'), may hold values from -6 to 6
- warm_right: bfloat16 [4, 4, 5, 4, 1024], P('row', 'col', None, None, 'mp'), may hold values from -6 to 6
Outputs:
- new_weights: bfloat16 [4, 4, 5, 2304, 1024], P('row', 'col', None, None, 'mp')
- next_down: float32 [4, 4, 5, 4, 1024], P('row', 'col', None, None, 'mp')
- next_right: float32 [4, 4, 5, 4, 1024], P('row', 'col', None, None, 'mp')
The draws below stay inside these ranges and needn't reach their ends.
All inputs are finite; a program needn't handle non-finite values.
Results may differ from the reference program's by a relative error of at most 0.0085.
Values may be sent and summed in bfloat16 or wider, within the bound.
No kernel may reach another device: no remote copies, remote signals or barrier semaphores. Data moves between devices by JAX's collectives and lax.ppermute only.
A program may use at most 128 MiB of HBM per device.

```python
import jax
import jax.numpy as jnp
from jax import lax

D = 2304
KVW = 1024
RANK = 4
LAYERS = 5
ROUNDS = 2
GRID_ROWS = 4
GRID_COLS = 4


def block_levels(key, dims, shards, smallest, high):
    factor_of, own = 1.0, jax.random.fold_in(key, 6)
    for dim, shards_of in shards:
        heights = jnp.exp(jax.random.uniform(jax.random.fold_in(own, dim), (shards_of,), jnp.float32, smallest / len(shards), high / len(shards)))
        factor_of = factor_of * jnp.repeat(heights, dims[dim] // shards_of).reshape([-1 if axis == dim else 1 for axis in range(len(dims))])
    return factor_of


def scatter_about(key, extent, width, bound, split=(), held_as=jnp.bfloat16):
    level = block_levels(key, extent, split, -0.22, 0.18) if split else 1.0
    array = jax.random.normal(key, extent, jnp.float32) * width * level
    return jnp.minimum(jnp.maximum(array, -bound), bound).astype(held_as)


def setup_inputs(seed: int = 0) -> dict:
    arg_keys = jax.random.split(jax.random.key(seed), 4)
    weights = scatter_about(arg_keys[0], (GRID_ROWS, GRID_COLS, LAYERS, D, KVW), 1.0, 6.0, ((0, 4), (1, 4), (4, 2)))
    warm_down = scatter_about(arg_keys[1], (GRID_ROWS, GRID_COLS, LAYERS, RANK, KVW), 1.0, 6.0, ((0, 4), (1, 4), (4, 2)))
    warm_right = scatter_about(arg_keys[2], (GRID_ROWS, GRID_COLS, LAYERS, RANK, KVW), 1.0, 6.0, ((0, 4), (1, 4), (4, 2)))
    return {"weights": weights, "warm_down": warm_down, "warm_right": warm_right}


step_size = 0.2
epsilon = 1e-06

def orthonormal(vectors):
    basis = []
    for column in range(vectors.shape[-2]):
        source = vectors[..., column, :]
        update = source
        for earlier in basis:
            update = update - lax.optimization_barrier(jnp.sum(source * earlier, axis=-1, keepdims=True)) * earlier
        basis.append(update / jnp.sqrt(lax.optimization_barrier(jnp.sum(update * update, axis=-1, keepdims=True)) + epsilon))
    return jnp.stack(basis, axis=-2)

def forward_products(layer_x, factors):

    def single(operands):
        return jnp.dot(operands[1], operands[0].T, preferred_element_type=jnp.float32)
    return lax.map(single, (layer_x, factors))

def backward_products(layer_x, basis):

    def single(operands):
        return jnp.dot(operands[1], operands[0], preferred_element_type=jnp.float32)
    return lax.map(single, (layer_x, basis))

def apply_update(layer_x, basis, factors):

    def single(triple):
        correction = jnp.dot(triple[1].T, triple[2], preferred_element_type=jnp.float32)
        return (triple[0].astype(jnp.float32) - step_size * correction).astype(jnp.bfloat16)
    return lax.map(single, (layer_x, basis, factors))

def one_round(layer_x, down_q, right_q):
    node_count = GRID_ROWS * GRID_COLS
    flat_x = layer_x.reshape(node_count, D, KVW)

    def to_grid(values):
        return values.reshape(GRID_ROWS, GRID_COLS, values.shape[1], values.shape[2])

    def to_flat(values):
        return values.reshape(node_count, values.shape[2], values.shape[3])
    stacked = jnp.concatenate([down_q, right_q, jnp.roll(down_q, 1, 0), jnp.roll(right_q, 1, 1)], axis=2)
    forward = to_grid(forward_products(flat_x, to_flat(stacked)))
    down_diff = forward[:, :, :RANK] - jnp.roll(forward[:, :, 2 * RANK:3 * RANK], -1, 0)
    right_diff = forward[:, :, RANK:2 * RANK] - jnp.roll(forward[:, :, 3 * RANK:], -1, 1)
    down_p = orthonormal(down_diff).astype(jnp.bfloat16)
    right_p = orthonormal(right_diff).astype(jnp.bfloat16)
    basis = jnp.concatenate([down_p, right_p, jnp.roll(down_p, 1, 0), jnp.roll(right_p, 1, 1)], axis=2)
    backward = to_grid(backward_products(flat_x, to_flat(basis)))
    down_c = backward[:, :, :RANK] - jnp.roll(backward[:, :, 2 * RANK:3 * RANK], -1, 0)
    right_c = backward[:, :, RANK:2 * RANK] - jnp.roll(backward[:, :, 3 * RANK:], -1, 1)
    down_next = down_c.astype(jnp.bfloat16)
    right_next = right_c.astype(jnp.bfloat16)
    own_basis = jnp.concatenate([down_p, right_p, -jnp.roll(down_p, 1, 0), -jnp.roll(right_p, 1, 1)], axis=2)
    own_factors = jnp.concatenate([down_next, right_next, jnp.roll(down_next, 1, 0), jnp.roll(right_next, 1, 1)], axis=2)
    new_x = apply_update(flat_x, to_flat(own_basis), to_flat(own_factors)).reshape(layer_x.shape)
    return (new_x, down_next, right_next, down_c, right_c)

def reference(weights, warm_down, warm_right):
    new_layers = []
    downs = []
    rights = []
    for level_index in range(LAYERS):
        layer_x = weights[:, :, level_index]
        down_q = warm_down[:, :, level_index]
        right_q = warm_right[:, :, level_index]
        down_c = jnp.zeros(down_q.shape, jnp.float32)
        right_c = jnp.zeros(right_q.shape, jnp.float32)
        for repeat in range(ROUNDS):
            layer_x, down_q, right_q, down_c, right_c = one_round(layer_x, down_q, right_q)
        new_layers.append(layer_x)
        downs.append(down_c)
        rights.append(right_c)
    return (jnp.stack(new_layers, 2), jnp.stack(downs, 2), jnp.stack(rights, 2))
```

```python
import functools

import jax
import jax.numpy as jnp
from jax import lax
from jax.experimental import pallas as pl
from jax.experimental.pallas import tpu as pltpu
from jax.sharding import PartitionSpec as P

ROUNDS = 2
step_size = 0.2
epsilon = 1e-06

BF16 = jnp.bfloat16
F32 = jnp.float32
MIB = 1024 * 1024


def passed_along(value, axis, by):
    devices = lax.axis_size(axis)
    return lax.ppermute(value, axis, [(i, (i + by) % devices) for i in range(devices)])


def from_partners(value, axis):
    return [passed_along(value, axis, by) for by in range(1, lax.axis_size(axis))]


def rows_by_features(left, right):
    return lax.dot_general(left, right, (((1,), (1,)), ((), ())), preferred_element_type=F32)


def in_two_parts(value):
    high = value.astype(BF16)
    low = (value - high.astype(F32)).astype(BF16)
    return jnp.concatenate([high, low], axis=0)


def small_times(small, wide):
    rows = small.shape[0]
    both = jnp.dot(in_two_parts(small), wide, preferred_element_type=F32)
    return both[:rows] + both[rows:]


def call(kernel, outs, args, arg_spaces, scratch=(), limit=16, flops=1_000_000, name=None):
    return pl.pallas_call(
        kernel,
        out_shape=[jax.ShapeDtypeStruct(shape, dtype) for shape, dtype, _ in outs],
        in_specs=[pl.BlockSpec(memory_space=space) for space in arg_spaces],
        out_specs=[pl.BlockSpec(memory_space=space) for _, _, space in outs],
        scratch_shapes=list(scratch),
        compiler_params=pltpu.CompilerParams(vmem_limit_bytes=limit * MIB),
        cost_estimate=pl.CostEstimate(flops=flops, bytes_accessed=0, transcendentals=0),
        name=name,
    )(*args)


def load_kernel(w_hbm, down_ref, right_ref, w_ref, own_ref, sems):
    count = w_ref.shape[0]
    copies = [pltpu.make_async_copy(w_hbm.at[l], w_ref.at[l], sems.at[l]) for l in range(count)]
    for copy in copies:
        copy.start()
    for l in range(count):
        copies[l].wait()
        factors = jnp.concatenate([down_ref[l], right_ref[l]], axis=0)
        own_ref[l] = rows_by_features(factors, w_ref[l])


def store_products(l, row, col, row_keep, row_send, col_keep, left_send, right_send):
    row_keep[l] = row
    row_send[l] = row.astype(BF16)
    col_keep[l] = col
    left_send[l] = col[:4].astype(BF16)
    right_send[l] = col[4:].astype(BF16)


def first_products_kernel(w_ref, up_ref, left_ref, own_ref, *outs):
    for l in range(w_ref.shape[0]):
        factors = jnp.concatenate([up_ref[l], left_ref[l]], axis=0)
        theirs = rows_by_features(factors, w_ref[l])
        own = own_ref[l]
        row = jnp.concatenate([theirs[:4], own[:4]], axis=0)
        col = jnp.concatenate([theirs[4:], own[4:]], axis=0)
        store_products(l, row, col, *outs)


def middle_kernel(partners, row_keep, col_keep, from_left, from_right, *refs):
    received, (row_total, up_send, down_send, col_diff, col_send) = refs[:partners], refs[partners:]
    for l in range(row_keep.shape[0]):
        row = row_keep[l]
        for other in received:
            row = row + other[l].astype(F32)
        row_total[l] = row
        up_send[l] = row[:4].astype(BF16)
        down_send[l] = row[4:].astype(BF16)
        col = col_keep[l] - jnp.concatenate([from_left[l], from_right[l]], axis=0).astype(F32)
        col_diff[l] = col
        col_send[l] = col.astype(BF16)


def orthonormal(vectors):
    rank = vectors.shape[0] // 2
    row = lax.broadcasted_iota(jnp.int32, (vectors.shape[0], 1), 0)
    first = row < rank
    place = jnp.where(first, row, row - rank)
    rest, basis = vectors, None
    for k in range(rank):
        current = jnp.where(first, rest[k : k + 1], rest[rank + k : rank + k + 1])
        square = jnp.sum(current * current, axis=1, keepdims=True)
        unit = current * (1.0 / jnp.sqrt(square + epsilon))
        basis = unit if basis is None else jnp.where(place == k, unit, basis)
        if k + 1 < rank:
            along = jnp.sum(vectors * unit, axis=1, keepdims=True)
            rest = rest - along * unit
    return basis


def back_kernel(partners, earlier, w_ref, row_total, from_above, from_below, col_diff, *refs):
    received, refs = refs[:partners], refs[partners:]
    pairs, refs = refs[: 2 * earlier], refs[2 * earlier :]
    basis_ref, back_ref, up_send, down_send, left_send, right_send = refs
    for l in range(w_ref.shape[0]):
        row = row_total[l] - jnp.concatenate([from_above[l], from_below[l]], axis=0).astype(F32)
        col = col_diff[l]
        for other in received:
            col = col + other[l].astype(F32)
        basis = jnp.concatenate([orthonormal(row), orthonormal(col)], axis=0).astype(BF16)
        basis_ref[l] = basis
        back = jnp.dot(basis, w_ref[l], preferred_element_type=F32)
        for e in range(earlier):
            mixing = rows_by_features(basis, pairs[2 * e][l])
            back = back + small_times(-step_size * mixing, pairs[2 * e + 1][l])
        back_ref[l] = back
        for i, send in enumerate((up_send, down_send, left_send, right_send)):
            send[l] = back[4 * i : 4 * i + 4].astype(BF16)


def combined_of(l, back_ref, above, below, left, right):
    theirs = jnp.concatenate([above[l], below[l], left[l], right[l]], axis=0)
    return back_ref[l] + theirs.astype(F32)


def next_products_kernel(earlier, w_ref, back_ref, above, below, left, right, *refs):
    bases, refs = refs[: earlier + 1], refs[earlier + 1 :]
    old_factors, refs = refs[:earlier], refs[earlier:]
    factors_ref, outs = refs[0], refs[1:]
    for l in range(w_ref.shape[0]):
        factors = combined_of(l, back_ref, above, below, left, right).astype(BF16)
        factors_ref[l] = factors
        products = rows_by_features(factors, w_ref[l])
        for e in range(earlier + 1):
            base_factors = old_factors[e][l] if e < earlier else factors
            mixing = rows_by_features(factors, base_factors)
            products = products + small_times(-step_size * mixing, bases[e][l])
        store_products(l, products[:8], products[8:], *outs)


def finish_kernel(earlier, chunk, w_ref, back_ref, above, below, left, right, *refs):
    bases, refs = refs[: earlier + 1], refs[earlier + 1 :]
    old_factors, refs = refs[:earlier], refs[earlier:]
    w_out, down_out, right_out, staged, sems = refs
    count, depth, _ = w_ref.shape
    copies = []
    for l in range(count):
        combined = combined_of(l, back_ref, above, below, left, right)
        down_out[l] = combined[4:8]
        right_out[l] = combined[12:]
        factors = jnp.concatenate([f[l] for f in old_factors] + [combined.astype(BF16)], axis=0)
        for c in range(depth // chunk):
            part = pl.ds(c * chunk, chunk)
            basis = jnp.concatenate([b[l, :, part] for b in bases], axis=0)
            correction = lax.dot_general(
                basis, factors, (((0,), (0,)), ((), ())), preferred_element_type=F32
            )
            staged[l, part] = (w_ref[l, part].astype(F32) - step_size * correction).astype(BF16)
            copy = pltpu.make_async_copy(
                staged.at[l, part], w_out.at[l, part], sems.at[l, c]
            )
            copy.start()
            copies.append(copy)
    for copy in copies:
        copy.wait()


def body(weights, warm_down, warm_right):
    vmem, hbm = pltpu.VMEM, pltpu.HBM
    w_hbm, down, right = weights[0, 0], warm_down[0, 0], warm_right[0, 0]
    w_hbm = pltpu.with_memory_space_constraint(w_hbm, pltpu.HBM)
    count, depth, width = w_hbm.shape
    rank = down.shape[1]
    partners = lax.axis_size("mp") - 1
    pair, every = 2 * rank, 4 * rank
    work = 2 * count * depth * width * every

    above = passed_along(down, "row", 1)
    beside = passed_along(right, "col", 1)
    w, own = call(
        load_kernel,
        [((count, depth, width), BF16, vmem), ((count, pair, depth), F32, vmem)],
        (w_hbm, down, right),
        (hbm, vmem, vmem),
        [pltpu.SemaphoreType.DMA((count,))],
        flops=10 * work,
        name="load",
    )
    product_outs = [
        ((count, pair, depth), F32, vmem),
        ((count, pair, depth), BF16, vmem),
        ((count, pair, depth), F32, vmem),
        ((count, rank, depth), BF16, vmem),
        ((count, rank, depth), BF16, vmem),
    ]
    products = call(
        first_products_kernel, product_outs, (w, above, beside, own), [vmem] * 4, name="first"
    )
    bases, factors = [], []
    for repeat in range(ROUNDS):
        row_keep, row_send, col_keep, left_send, right_send = products
        received = from_partners(row_send, "mp")
        from_left = passed_along(right_send, "col", 1)
        from_right = passed_along(left_send, "col", -1)
        args = (row_keep, col_keep, from_left, from_right, *received)
        row_total, up_send, down_send, col_diff, col_send = call(
            functools.partial(middle_kernel, partners),
            [
                ((count, pair, depth), F32, vmem),
                ((count, rank, depth), BF16, vmem),
                ((count, rank, depth), BF16, vmem),
                ((count, pair, depth), F32, vmem),
                ((count, pair, depth), BF16, vmem),
            ],
            args,
            [vmem] * len(args),
            name=f"middle_{repeat}",
        )
        from_above = passed_along(down_send, "row", 1)
        from_below = passed_along(up_send, "row", -1)
        received = from_partners(col_send, "mp")
        pairs = [x for both in zip(bases, factors) for x in both]
        args = (w, row_total, from_above, from_below, col_diff, *received, *pairs)
        basis, back, up_send, down_send, left_send, right_send = call(
            functools.partial(back_kernel, partners, repeat),
            [((count, every, depth), BF16, vmem), ((count, every, width), F32, vmem)]
            + [((count, rank, width), BF16, vmem)] * 4,
            args,
            [vmem] * len(args),
            name=f"back_{repeat}",
        )
        bases = bases + [basis]
        from_above = passed_along(down_send, "row", 1)
        from_below = passed_along(up_send, "row", -1)
        from_left = passed_along(right_send, "col", 1)
        from_right = passed_along(left_send, "col", -1)
        args = (w, back, from_above, from_below, from_left, from_right, *bases, *factors)
        if repeat + 1 < ROUNDS:
            out = call(
                functools.partial(next_products_kernel, repeat),
                [((count, every, width), BF16, vmem)] + product_outs,
                args,
                [vmem] * len(args),
                name=f"next_{repeat}",
            )
            factors, products = factors + [out[0]], out[1:]
    chunk = depth // 3 if depth % 384 == 0 else depth
    new_w, next_down, next_right = call(
        functools.partial(finish_kernel, ROUNDS - 1, chunk),
        [
            ((count, depth, width), BF16, hbm),
            ((count, rank, width), F32, vmem),
            ((count, rank, width), F32, vmem),
        ],
        args,
        [vmem] * len(args),
        [
            pltpu.VMEM((count, depth, width), BF16),
            pltpu.SemaphoreType.DMA((count, depth // chunk)),
        ],
        limit=28,
        name="finish",
    )
    return new_w[None, None], next_down[None, None], next_right[None, None]


def solution(mesh):
    placed = (P("row", "col", None, None, "mp"),) * 3
    return jax.shard_map(
        body, mesh=mesh, in_specs=placed, out_specs=placed, check_vma=False
    )
```

```python
import functools

import jax
import jax.numpy as jnp
from jax import lax
from jax.experimental import pallas as pl
from jax.experimental.pallas import tpu as pltpu
from jax.sharding import PartitionSpec as P


ROUNDS = 2
step_size = 0.2
epsilon = 1e-06

BF16 = jnp.bfloat16
F32 = jnp.float32
MIB = 1024 * 1024


def passed_along(value, axis, by):
    devices = lax.axis_size(axis)
    return lax.ppermute(value, axis, [(i, (i + by) % devices) for i in range(devices)])


def from_partners(value, axis):
    return [passed_along(value, axis, by) for by in range(1, lax.axis_size(axis))]


def rows_by_features(left, right):
    return lax.dot_general(left, right, (((1,), (1,)), ((), ())), preferred_element_type=F32)


def in_two_parts(value):
    high = value.astype(BF16)
    low = (value - high.astype(F32)).astype(BF16)
    return jnp.concatenate([high, low], axis=0)


def small_times(small, wide):
    rows = small.shape[0]
    both = jnp.dot(in_two_parts(small), wide, preferred_element_type=F32)
    return both[:rows] + both[rows:]


def call(kernel, outs, args, arg_spaces, scratch=(), limit=16, flops=1_000_000):
    return pl.pallas_call(
        kernel,
        out_shape=[jax.ShapeDtypeStruct(shape, dtype) for shape, dtype, _ in outs],
        in_specs=[pl.BlockSpec(memory_space=space) for space in arg_spaces],
        out_specs=[pl.BlockSpec(memory_space=space) for _, _, space in outs],
        scratch_shapes=list(scratch),
        compiler_params=pltpu.CompilerParams(vmem_limit_bytes=limit * MIB),
        cost_estimate=pl.CostEstimate(flops=flops, bytes_accessed=0, transcendentals=0),
    )(*args)


def store_products(l, row, col, row_keep, row_send, col_keep, left_send, right_send):
    row_keep[l] = row
    row_send[l] = row.astype(BF16)
    col_keep[l] = col
    left_send[l] = col[:4].astype(BF16)
    right_send[l] = col[4:].astype(BF16)


def layer_of(w_refs, l):
    early = w_refs[0].shape[0]
    return (w_refs[0], l) if l < early else (w_refs[1], l - early)


def load_kernel(w_hbm, down_hbm, right_hbm, w_ref, down_ref, right_ref, sems):
    copies = [
        pltpu.make_async_copy(down_hbm, down_ref, sems.at[0]),
        pltpu.make_async_copy(right_hbm, right_ref, sems.at[1]),
    ]
    for l in range(w_ref.shape[0]):
        copies.append(pltpu.make_async_copy(w_hbm.at[l], w_ref.at[l], sems.at[2 + l]))
    for copy in copies:
        copy.start()
    for copy in copies:
        copy.wait()


def first_products_kernel(w_hbm, w_early, up_ref, down_ref, left_ref, right_ref, *refs):
    w_late, *outs, sems = refs
    early, late = w_early.shape[0], w_late.shape[0]
    copies = [
        pltpu.make_async_copy(w_hbm.at[early + l], w_late.at[l], sems.at[l]) for l in range(late)
    ]
    for copy in copies:
        copy.start()
    for l in range(early + late):
        if l >= early:
            copies[l - early].wait()
        ref, at = layer_of((w_early, w_late), l)
        factors = jnp.concatenate([up_ref[l], down_ref[l], left_ref[l], right_ref[l]], axis=0)
        products = rows_by_features(factors, ref[at])
        store_products(l, products[:8], products[8:], *outs)


def middle_col_kernel(col_keep, from_left, from_right, col_diff, col_send):
    for l in range(col_keep.shape[0]):
        col = col_keep[l] - jnp.concatenate([from_left[l], from_right[l]], axis=0).astype(F32)
        col_diff[l] = col
        col_send[l] = col.astype(BF16)


def middle_row_kernel(partners, row_keep, *refs):
    received, (row_total, up_send, down_send) = refs[:partners], refs[partners:]
    for l in range(row_keep.shape[0]):
        row = row_keep[l]
        for other in received:
            row = row + other[l].astype(F32)
        row_total[l] = row
        up_send[l] = row[:4].astype(BF16)
        down_send[l] = row[4:].astype(BF16)


def orthonormal(vectors):
    rank = vectors.shape[0] // 2
    row = lax.broadcasted_iota(jnp.int32, (vectors.shape[0], 1), 0)
    first = row < rank
    place = jnp.where(first, row, row - rank)
    rest, basis = vectors, None
    for k in range(rank):
        current = jnp.where(first, rest[k : k + 1], rest[rank + k : rank + k + 1])
        square = jnp.sum(current * current, axis=1, keepdims=True)
        unit = current * (1.0 / jnp.sqrt(square + epsilon))
        basis = unit if basis is None else jnp.where(place == k, unit, basis)
        if k + 1 < rank:
            along = jnp.sum(vectors * unit, axis=1, keepdims=True)
            rest = rest - along * unit
    return basis


def back_product(l, vectors, earlier, w_refs, pairs, basis_ref, back_ref, sends):
    basis = orthonormal(vectors).astype(BF16)
    basis_ref[l] = basis
    ref, at = layer_of(w_refs, l)
    back = jnp.dot(basis, ref[at], preferred_element_type=F32)
    for e in range(earlier):
        row_basis, col_basis, old_factors = (ref[l] for ref in pairs[3 * e : 3 * e + 3])
        mixing = rows_by_features(basis, jnp.concatenate([row_basis, col_basis], axis=0))
        back = back + small_times(-step_size * mixing, old_factors)
    back_ref[l] = back
    for i, send in enumerate(sends):
        send[l] = back[4 * i : 4 * i + 4].astype(BF16)


def back_col_kernel(partners, earlier, w_early, w_late, col_diff, *refs):
    received, refs = refs[:partners], refs[partners:]
    pairs, (basis_ref, back_ref, *sends) = refs[: 3 * earlier], refs[3 * earlier :]
    for l in range(col_diff.shape[0]):
        col = col_diff[l]
        for other in received:
            col = col + other[l].astype(F32)
        back_product(l, col, earlier, (w_early, w_late), pairs, basis_ref, back_ref, sends)


def back_row_kernel(earlier, w_early, w_late, row_total, from_above, from_below, *refs):
    pairs, (basis_ref, back_ref, *sends) = refs[: 3 * earlier], refs[3 * earlier :]
    for l in range(row_total.shape[0]):
        row = row_total[l] - jnp.concatenate([from_above[l], from_below[l]], axis=0).astype(F32)
        back_product(l, row, earlier, (w_early, w_late), pairs, basis_ref, back_ref, sends)


def combined_of(l, row_back, col_back, above, below, left, right):
    own = jnp.concatenate([row_back[l], col_back[l]], axis=0)
    theirs = jnp.concatenate([above[l], below[l], left[l], right[l]], axis=0)
    return own + theirs.astype(F32)


def next_products_kernel(earlier, w_early, w_late, *refs):
    moved, refs = refs[:6], refs[6:]
    pairs, refs = refs[: 3 * earlier], refs[3 * earlier :]
    row_basis, col_basis, factors_ref, *outs = refs
    for l in range(factors_ref.shape[0]):
        factors = combined_of(l, *moved).astype(BF16)
        factors_ref[l] = factors
        ref, at = layer_of((w_early, w_late), l)
        products = rows_by_features(factors, ref[at])
        known = [tuple(ref[l] for ref in pairs[3 * e : 3 * e + 3]) for e in range(earlier)]
        for row, col, old in known + [(row_basis[l], col_basis[l], factors)]:
            mixing = rows_by_features(factors, old)
            products = products + small_times(
                -step_size * mixing, jnp.concatenate([row, col], axis=0)
            )
        store_products(l, products[:8], products[8:], *outs)


def finish_kernel(earlier, chunk, w_early, w_late, *refs):
    moved, refs = refs[:6], refs[6:]
    pairs, refs = refs[: 3 * earlier], refs[3 * earlier :]
    row_basis, col_basis, w_out, down_out, right_out, staged, sems = refs
    bases = [pairs[3 * e + i] for e in range(earlier) for i in (0, 1)] + [row_basis, col_basis]
    count, depth, _ = staged.shape
    copies = []
    for l in range(count):
        combined = combined_of(l, *moved)
        down_out[l] = combined[4:8]
        right_out[l] = combined[12:]
        old_factors = [pairs[3 * e + 2][l] for e in range(earlier)]
        factors = jnp.concatenate(old_factors + [combined.astype(BF16)], axis=0)
        ref, at = layer_of((w_early, w_late), l)
        for c in range(depth // chunk):
            part = pl.ds(c * chunk, chunk)
            basis = jnp.concatenate([b[l, :, part] for b in bases], axis=0)
            correction = lax.dot_general(
                basis, factors, (((0,), (0,)), ((), ())), preferred_element_type=F32
            )
            staged[l, part] = (ref[at, part].astype(F32) - step_size * correction).astype(BF16)
            copy = pltpu.make_async_copy(
                staged.at[l, part], w_out.at[l, part], sems.at[l, c]
            )
            copy.start()
            copies.append(copy)
    for copy in copies:
        copy.wait()


def body(weights, warm_down, warm_right):
    vmem, hbm = pltpu.VMEM, pltpu.HBM
    w, down, right = weights[0, 0], warm_down[0, 0], warm_right[0, 0]
    count, depth, width = w.shape
    rank = down.shape[1]
    partners = lax.axis_size("mp") - 1
    pair, every = 2 * rank, 4 * rank

    def local(kernel, outs, args, **more):
        return call(kernel, outs, args, [vmem] * len(args), **more)

    kept = ((count, pair, depth), F32, vmem)
    both_edges = ((count, pair, depth), BF16, vmem)
    one_edge = ((count, rank, depth), BF16, vmem)
    product_outs = [kept, both_edges, kept, one_edge, one_edge]
    back_outs = [both_edges, ((count, pair, width), F32, vmem)]
    back_outs += [((count, rank, width), BF16, vmem)] * 2

    above = passed_along(down, "row", 1)
    beside = passed_along(right, "col", 1)
    w_hbm, down_hbm, right_hbm = (
        pltpu.with_memory_space_constraint(x, pltpu.HBM) for x in (w, down, right)
    )
    early = max(1, 2 * count // 5)
    own_factors = ((count, rank, width), BF16, vmem)
    w_early, own_down, own_right = call(
        load_kernel,
        [((early, depth, width), BF16, vmem), own_factors, own_factors],
        (w_hbm, down_hbm, right_hbm),
        [hbm] * 3,
        [pltpu.SemaphoreType.DMA((early + 2,))],
        flops=100_000_000,
    )
    w_late, *products = call(
        first_products_kernel,
        [((count - early, depth, width), BF16, vmem)] + product_outs,
        (w_hbm, w_early, above, own_down, beside, own_right),
        [hbm] + [vmem] * 5,
        [pltpu.SemaphoreType.DMA((count - early,))],
    )
    w = (w_early, w_late)
    pairs = ()
    for repeat in range(ROUNDS):
        row_keep, row_send, col_keep, left_send, right_send = products
        row_received = from_partners(row_send, "mp")
        from_left = passed_along(right_send, "col", 1)
        from_right = passed_along(left_send, "col", -1)
        col_diff, col_send = local(
            middle_col_kernel, [kept, both_edges], (col_keep, from_left, from_right),
        )
        col_received = from_partners(col_send, "mp")
        row_total, up_send, down_send = local(
            functools.partial(middle_row_kernel, partners),
            [kept, one_edge, one_edge], (row_keep, *row_received),
        )
        from_above = passed_along(down_send, "row", 1)
        from_below = passed_along(up_send, "row", -1)
        col_basis, col_back, left_send, right_send = local(
            functools.partial(back_col_kernel, partners, repeat),
            back_outs, (*w, col_diff, *col_received, *pairs),
        )
        from_left = passed_along(right_send, "col", 1)
        from_right = passed_along(left_send, "col", -1)
        row_basis, row_back, up_send, down_send = local(
            functools.partial(back_row_kernel, repeat),
            back_outs, (*w, row_total, from_above, from_below, *pairs),
        )
        from_above = passed_along(down_send, "row", 1)
        from_below = passed_along(up_send, "row", -1)
        moved = (row_back, col_back, from_above, from_below, from_left, from_right)
        args = (*w, *moved, *pairs, row_basis, col_basis)
        if repeat + 1 < ROUNDS:
            factors, *products = local(
                functools.partial(next_products_kernel, repeat),
                [((count, every, width), BF16, vmem)] + product_outs, args,
            )
            pairs = (*pairs, row_basis, col_basis, factors)
    chunk = depth // 3 if depth % 384 == 0 else depth
    new_w, next_down, next_right = local(
        functools.partial(finish_kernel, ROUNDS - 1, chunk),
        [
            ((count, depth, width), BF16, hbm),
            ((count, rank, width), F32, vmem),
            ((count, rank, width), F32, vmem),
        ],
        args,
        scratch=[
            pltpu.VMEM((count, depth, width), BF16),
            pltpu.SemaphoreType.DMA((count, depth // chunk)),
        ],
        limit=28,
    )
    return new_w[None, None], next_down[None, None], next_right[None, None]


def solution(mesh):
    placed = (P("row", "col", None, None, "mp"),) * 3
    return jax.shard_map(body, mesh=mesh, in_specs=placed, out_specs=placed, check_vma=False)
```

```python
import functools

import jax
import jax.numpy as jnp
from jax import lax
from jax.experimental import pallas as pl
from jax.experimental.pallas import tpu as pltpu
from jax.sharding import PartitionSpec as P


ROUNDS = 2
step_size = 0.2
epsilon = 1e-06

BF16 = jnp.bfloat16
F32 = jnp.float32
MIB = 1024 * 1024


def passed_along(value, axis, by):
    devices = lax.axis_size(axis)
    return lax.ppermute(value, axis, [(i, (i + by) % devices) for i in range(devices)])


def from_partners(value, axis):
    return [passed_along(value, axis, by) for by in range(1, lax.axis_size(axis))]


def call(kernel, outs, args, arg_spaces, scratch=(), limit=16, flops=1_000_000):
    return pl.pallas_call(
        kernel,
        out_shape=[jax.ShapeDtypeStruct(shape, dtype) for shape, dtype, _ in outs],
        in_specs=[pl.BlockSpec(memory_space=space) for space in arg_spaces],
        out_specs=[pl.BlockSpec(memory_space=space) for _, _, space in outs],
        scratch_shapes=list(scratch),
        compiler_params=pltpu.CompilerParams(vmem_limit_bytes=limit * MIB),
        cost_estimate=pl.CostEstimate(flops=flops, bytes_accessed=0, transcendentals=0),
    )(*args)


def rows_by_features(left, right):
    return lax.dot_general(left, right, (((1,), (1,)), ((), ())), preferred_element_type=F32)


def layer_of(w_refs, l):
    for ref in w_refs:
        if l < ref.shape[0]:
            return ref, l
        l -= ref.shape[0]


def within_layers(mixing, pair):
    rows, cols = mixing.shape
    row = lax.broadcasted_iota(jnp.int32, (rows, cols), 0)
    col = lax.broadcasted_iota(jnp.int32, (rows, cols), 1)
    stack = cols // 2
    row = jnp.where(row < stack, row, row - stack) // pair
    col = jnp.where(col < stack, col, col - stack) // pair
    return jnp.where(row == col, -step_size * mixing, 0.0)


def small_times(small, wide):
    high = small.astype(BF16)
    low = (small - high.astype(F32)).astype(BF16)
    both = jnp.dot(jnp.concatenate([high, low], axis=0), wide, preferred_element_type=F32)
    return both[: small.shape[0]] + both[small.shape[0] :]


def load_kernel(w_hbm, down_hbm, right_hbm, w_ref, down_ref, right_ref, sems):
    copies = [
        pltpu.make_async_copy(down_hbm, down_ref, sems.at[0]),
        pltpu.make_async_copy(right_hbm, right_ref, sems.at[1]),
    ]
    for l in range(w_ref.shape[0]):
        copies.append(pltpu.make_async_copy(w_hbm.at[l], w_ref.at[l], sems.at[2 + l]))
    for copy in copies:
        copy.start()
    for copy in copies:
        copy.wait()


def load_more_kernel(start, w_hbm, w_ref, sems):
    copies = [
        pltpu.make_async_copy(w_hbm.at[start + l], w_ref.at[l], sems.at[l])
        for l in range(w_ref.shape[0])
    ]
    for copy in copies:
        copy.start()
    for copy in copies:
        copy.wait()


def store_products(l, row, col, row_keep, up_send, down_send, col_keep, col_send):
    rank = row.shape[0] // 2
    row_keep[l] = row
    up_send[l] = row[:rank].astype(BF16)
    down_send[l] = row[rank:].astype(BF16)
    col_keep[l] = col
    col_send[l] = col.astype(BF16)


def first_products_kernel(w_hbm, w_a, w_b, up_ref, down_ref, left_ref, right_ref, *refs):
    w_c, *outs, sems = refs
    early, late = w_a.shape[0] + w_b.shape[0], w_c.shape[0]
    copies = [
        pltpu.make_async_copy(w_hbm.at[early + l], w_c.at[l], sems.at[l]) for l in range(late)
    ]
    for copy in copies:
        copy.start()
    for l in range(early + late):
        if l >= early:
            copies[l - early].wait()
        ref, at = layer_of((w_a, w_b, w_c), l)
        factors = jnp.concatenate([up_ref[l], down_ref[l], left_ref[l], right_ref[l]], axis=0)
        products = rows_by_features(factors, ref[at])
        half = products.shape[0] // 2
        store_products(l, products[:half], products[half:], *outs)


def middle_col_kernel(partners, col_keep, *refs):
    received, (col_total, left_send, right_send) = refs[:partners], refs[partners:]
    rank = left_send.shape[1]
    for l in range(col_keep.shape[0]):
        col = col_keep[l]
        for other in received:
            col = col + other[l].astype(F32)
        col_total[l] = col
        left_send[l] = col[:rank].astype(BF16)
        right_send[l] = col[rank:].astype(BF16)


def middle_row_kernel(row_keep, from_above, from_below, row_diff, row_send):
    for l in range(row_keep.shape[0]):
        row = row_keep[l] - jnp.concatenate([from_above[l], from_below[l]], axis=0).astype(F32)
        row_diff[l] = row
        row_send[l] = row.astype(BF16)


def lane_sum(parts):
    total = parts[0]
    for part in parts[1:]:
        total = total + part
    return jnp.sum(total, axis=1, keepdims=True)


def orthonormal(v_ref, rank):
    tiles, stack, _ = v_ref.shape
    groups = stack // rank

    def vector(k):
        return [v_ref[t, pl.ds(k, groups, stride=rank), :] for t in range(tiles)]

    rest = [vector(k) for k in range(rank)]
    for k in range(rank):
        u = rest[k]
        square = lane_sum([x * x for x in u]) + epsilon
        for j in range(k + 1, rank):
            along = lane_sum([x * y for x, y in zip(vector(j), u)]) / square
            rest[j] = [x - along * y for x, y in zip(rest[j], u)]
        scale = 1.0 / jnp.sqrt(square)
        rest[k] = [x * scale for x in u]
    for k in range(rank):
        for t in range(tiles):
            v_ref[t, pl.ds(k, groups, stride=rank), :] = rest[k][t]


def store_vectors(v_ref, rows, values):
    for t in range(v_ref.shape[0]):
        v_ref[t, rows, :] = values[:, 128 * t : 128 * (t + 1)]


def back_products(v_ref, w_refs, pairs, basis_ref, back_ref, sends, layers):
    tiles, stack, _ = v_ref.shape
    pair = stack // layers
    rank = pair // 2
    orthonormal(v_ref, rank)
    basis = jnp.concatenate([v_ref[t] for t in range(tiles)], axis=1)
    basis_ref[...] = basis.astype(BF16)
    changes = None
    for old_basis, old_factors in pairs:
        mixing = within_layers(rows_by_features(basis.astype(BF16), old_basis[...]), pair)
        change = small_times(mixing, old_factors[...])
        changes = change if changes is None else changes + change
    for l in range(layers):
        here = slice(l * pair, (l + 1) * pair)
        ref, at = layer_of(w_refs, l)
        back = jnp.dot(basis[here].astype(BF16), ref[at], preferred_element_type=F32)
        if changes is not None:
            back = back + changes[here]
        back_ref[here, :] = back
        for i, send in enumerate(sends):
            send[l] = back[rank * i : rank * i + rank].astype(BF16)


def back_col_kernel(earlier, w_a, w_b, w_c, col_total, from_left, from_right, *refs):
    pairs, refs = refs[: 2 * earlier], refs[2 * earlier :]
    basis_ref, back_ref, *sends, v_ref = refs
    layers, pair, _ = col_total.shape
    for l in range(layers):
        theirs = jnp.concatenate([from_left[l], from_right[l]], axis=0).astype(F32)
        store_vectors(v_ref, slice(l * pair, (l + 1) * pair), col_total[l] - theirs)
    pairs = list(zip(pairs[::2], pairs[1::2]))
    back_products(v_ref, (w_a, w_b, w_c), pairs, basis_ref, back_ref, sends, layers)


def back_row_kernel(partners, earlier, w_a, w_b, w_c, row_diff, *refs):
    received, refs = refs[:partners], refs[partners:]
    pairs, refs = refs[: 2 * earlier], refs[2 * earlier :]
    basis_ref, back_ref, *sends, v_ref = refs
    layers, pair, _ = row_diff.shape
    for l in range(layers):
        row = row_diff[l]
        for other in received:
            row = row + other[l].astype(F32)
        store_vectors(v_ref, slice(l * pair, (l + 1) * pair), row)
    pairs = list(zip(pairs[::2], pairs[1::2]))
    back_products(v_ref, (w_a, w_b, w_c), pairs, basis_ref, back_ref, sends, layers)


def combined_of(l, back_ref, first, second):
    pair = 2 * first.shape[1]
    theirs = jnp.concatenate([first[l], second[l]], axis=0)
    return back_ref[l * pair : (l + 1) * pair, :] + theirs.astype(F32)


def next_products_kernel(earlier, w_a, w_b, w_c, *refs):
    (row_back, col_back, above, below, left, right), refs = refs[:6], refs[6:]
    pairs, refs = refs[: 2 * earlier], refs[2 * earlier :]
    row_basis, col_basis, bases_ref, factors_ref, *outs, f_ref = refs
    layers, rank, _ = above.shape
    pair, stack = 2 * rank, row_basis.shape[0]
    bases_ref[:stack, :] = row_basis[...]
    bases_ref[stack:, :] = col_basis[...]
    for l in range(layers):
        f_ref[l * pair : (l + 1) * pair, :] = combined_of(l, row_back, above, below)
        f_ref[stack + l * pair : stack + (l + 1) * pair, :] = combined_of(l, col_back, left, right)
    factors = f_ref[...].astype(BF16)
    factors_ref[...] = factors
    known = list(zip(pairs[::2], pairs[1::2])) + [(bases_ref, factors_ref)]
    changes = None
    for old_basis, old_factors in known:
        mixing = within_layers(rows_by_features(factors, old_factors[...]), pair)
        change = small_times(mixing, old_basis[...])
        changes = change if changes is None else changes + change
    for l in range(layers):
        row_at = slice(l * pair, (l + 1) * pair)
        col_at = slice(stack + l * pair, stack + (l + 1) * pair)
        own = jnp.concatenate([f_ref[row_at, :], f_ref[col_at, :]], axis=0).astype(BF16)
        ref, at = layer_of((w_a, w_b, w_c), l)
        products = rows_by_features(own, ref[at])
        store_products(
            l, products[:pair] + changes[row_at], products[pair:] + changes[col_at], *outs
        )


def finish_kernel(earlier, chunk, w_a, w_b, w_c, *refs):
    (row_back, col_back, above, below, left, right), refs = refs[:6], refs[6:]
    pairs, refs = refs[: 2 * earlier], refs[2 * earlier :]
    row_basis, col_basis, w_out, down_out, right_out, staged, sems = refs
    layers, depth, _ = staged.shape
    rank, stack = above.shape[1], row_basis.shape[0]
    pair = 2 * rank
    copies = []
    for l in range(layers):
        row_at = slice(l * pair, (l + 1) * pair)
        col_at = slice(stack + l * pair, stack + (l + 1) * pair)
        row = combined_of(l, row_back, above, below)
        col = combined_of(l, col_back, left, right)
        down_out[l] = row[rank:]
        right_out[l] = col[rank:]
        old = [f[at, :] for f in pairs[1::2] for at in (row_at, col_at)]
        factors = jnp.concatenate(old + [row.astype(BF16), col.astype(BF16)], axis=0)
        ref, at = layer_of((w_a, w_b, w_c), l)
        for c in range(depth // chunk):
            part = slice(c * chunk, (c + 1) * chunk)
            old = [b[rows, part] for b in pairs[::2] for rows in (row_at, col_at)]
            basis = jnp.concatenate(
                old + [row_basis[row_at, part], col_basis[row_at, part]], axis=0
            )
            correction = lax.dot_general(
                basis, factors, (((0,), (0,)), ((), ())), preferred_element_type=F32
            )
            staged[l, part] = (ref[at, part].astype(F32) - step_size * correction).astype(BF16)
            copy = pltpu.make_async_copy(staged.at[l, part], w_out.at[l, part], sems.at[l, c])
            copy.start()
            copies.append(copy)
    for copy in copies:
        copy.wait()


def body(weights, warm_down, warm_right):
    vmem, hbm = pltpu.VMEM, pltpu.HBM
    w_hbm, down_hbm, right_hbm = (
        pltpu.with_memory_space_constraint(x[0, 0], hbm) for x in (weights, warm_down, warm_right)
    )
    count, depth, width = w_hbm.shape
    rank = down_hbm.shape[1]
    partners = lax.axis_size("mp") - 1
    pair, stack = 2 * rank, 2 * rank * count
    dma = pltpu.SemaphoreType.DMA

    def local(kernel, outs, args, **more):
        return call(kernel, outs, args, [vmem] * len(args), **more)

    kept = ((count, pair, depth), F32, vmem)
    both_edges = ((count, pair, depth), BF16, vmem)
    one_edge = ((count, rank, depth), BF16, vmem)
    product_outs = [kept, one_edge, one_edge, kept, both_edges]
    own_factors = ((count, rank, width), BF16, vmem)
    back_outs = [((stack, depth), BF16, vmem), ((stack, width), F32, vmem), own_factors, own_factors]
    vectors = [pltpu.VMEM((depth // 128, stack, 128), F32)]

    some, more = max(1, count // 5), max(1, 2 * count // 5)
    w_a, own_down, own_right = call(
        load_kernel,
        [((some, depth, width), BF16, vmem), own_factors, own_factors],
        (w_hbm, down_hbm, right_hbm),
        [hbm] * 3,
        scratch=[dma((some + 2,))],
    )
    above = passed_along(own_down, "row", 1)
    beside = passed_along(own_right, "col", 1)
    (w_b,) = call(
        functools.partial(load_more_kernel, some),
        [((more, depth, width), BF16, vmem)],
        (w_hbm,),
        [hbm],
        scratch=[dma((more,))],
        flops=100_000_000,
    )
    rest = count - some - more
    w_c, *products = call(
        first_products_kernel,
        [((rest, depth, width), BF16, vmem)] + product_outs,
        (w_hbm, w_a, w_b, above, own_down, beside, own_right),
        [hbm] + [vmem] * 6,
        scratch=[dma((rest,))],
    )
    w = (w_a, w_b, w_c)
    pairs = ()
    for repeat in range(ROUNDS):
        row_keep, up_send, down_send, col_keep, col_send = products
        col_received = from_partners(col_send, "mp")
        from_above = passed_along(down_send, "row", 1)
        from_below = passed_along(up_send, "row", -1)
        col_total, left_send, right_send = local(
            functools.partial(middle_col_kernel, partners),
            [kept, one_edge, one_edge],
            (col_keep, *col_received),
        )
        from_left = passed_along(right_send, "col", 1)
        from_right = passed_along(left_send, "col", -1)
        row_diff, row_send = local(
            middle_row_kernel, [kept, both_edges], (row_keep, from_above, from_below)
        )
        row_received = from_partners(row_send, "mp")
        col_basis, col_back, left_send, right_send = local(
            functools.partial(back_col_kernel, repeat),
            back_outs,
            (*w, col_total, from_left, from_right, *pairs),
            scratch=vectors,
        )
        from_left = passed_along(right_send, "col", 1)
        from_right = passed_along(left_send, "col", -1)
        row_basis, row_back, up_send, down_send = local(
            functools.partial(back_row_kernel, partners, repeat),
            back_outs,
            (*w, row_diff, *row_received, *pairs),
            scratch=vectors,
        )
        from_above = passed_along(down_send, "row", 1)
        from_below = passed_along(up_send, "row", -1)
        moved = (row_back, col_back, from_above, from_below, from_left, from_right)
        args = (*w, *moved, *pairs, row_basis, col_basis)
        if repeat + 1 < ROUNDS:
            bases, factors, *products = local(
                functools.partial(next_products_kernel, repeat),
                [((2 * stack, depth), BF16, vmem), ((2 * stack, width), BF16, vmem)] + product_outs,
                args,
                scratch=[pltpu.VMEM((2 * stack, width), F32)],
            )
            pairs = (*pairs, bases, factors)
    chunk = depth // 3 if depth % 384 == 0 else depth
    new_w, next_down, next_right = local(
        functools.partial(finish_kernel, ROUNDS - 1, chunk),
        [
            ((count, depth, width), BF16, hbm),
            ((count, rank, width), F32, vmem),
            ((count, rank, width), F32, vmem),
        ],
        args,
        scratch=[pltpu.VMEM((count, depth, width), BF16), dma((count, depth // chunk))],
        limit=28,
    )
    return new_w[None, None], next_down[None, None], next_right[None, None]


def solution(mesh):
    placed = (P("row", "col", None, None, "mp"),) * 3
    return jax.shard_map(body, mesh=mesh, in_specs=placed, out_specs=placed, check_vma=False)
```

```python
import functools

import jax
import jax.numpy as jnp
from jax import lax
from jax.experimental import pallas as pl
from jax.experimental.pallas import tpu as pltpu
from jax.sharding import PartitionSpec as P


ROUNDS = 2
step_size = 0.2
epsilon = 1e-06

BF16 = jnp.bfloat16
F32 = jnp.float32
MIB = 1024 * 1024


def passed_along(value, axis, by):
    devices = lax.axis_size(axis)
    return lax.ppermute(value, axis, [(i, (i + by) % devices) for i in range(devices)])


def exchanged(value, axis, place):
    devices = lax.axis_size(axis)
    pairs = []
    for i in range(place, devices, 2):
        pairs += [(i, (i + 1) % devices), ((i + 1) % devices, i)]
    return lax.ppermute(value, axis, sorted(pairs))


def is_even(axis):
    return lax.rem(lax.axis_index(axis), 2) == 0


def from_partners(value, axis):
    return [passed_along(value, axis, by) for by in range(1, lax.axis_size(axis))]


def call(kernel, outs, args, arg_spaces, scratch=(), limit=16, flops=1_000_000):
    return pl.pallas_call(
        kernel,
        out_shape=[jax.ShapeDtypeStruct(shape, dtype) for shape, dtype, _ in outs],
        in_specs=[pl.BlockSpec(memory_space=space) for space in arg_spaces],
        out_specs=[pl.BlockSpec(memory_space=space) for _, _, space in outs],
        scratch_shapes=list(scratch),
        compiler_params=pltpu.CompilerParams(vmem_limit_bytes=limit * MIB),
        cost_estimate=pl.CostEstimate(flops=flops, bytes_accessed=0, transcendentals=0),
    )(*args)


def rows_by_features(left, right):
    return lax.dot_general(left, right, (((1,), (1,)), ((), ())), preferred_element_type=F32)


def layer_of(w_refs, l):
    for ref in w_refs:
        if l < ref.shape[0]:
            return ref, l
        l -= ref.shape[0]


def within_layers(mixing, pair):
    rows, cols = mixing.shape
    row = lax.broadcasted_iota(jnp.int32, (rows, cols), 0)
    col = lax.broadcasted_iota(jnp.int32, (rows, cols), 1)
    stack = cols // 2
    row = jnp.where(row < stack, row, row - stack) // pair
    col = jnp.where(col < stack, col, col - stack) // pair
    return jnp.where(row == col, -step_size * mixing, 0.0)


def small_times(small, wide):
    high = small.astype(BF16)
    low = (small - high.astype(F32)).astype(BF16)
    both = jnp.dot(jnp.concatenate([high, low], axis=0), wide, preferred_element_type=F32)
    return both[: small.shape[0]] + both[small.shape[0] :]


def load_kernel(w_hbm, down_hbm, right_hbm, w_ref, down_ref, right_ref, sems):
    copies = [
        pltpu.make_async_copy(down_hbm, down_ref, sems.at[0]),
        pltpu.make_async_copy(right_hbm, right_ref, sems.at[1]),
    ]
    for l in range(w_ref.shape[0]):
        copies.append(pltpu.make_async_copy(w_hbm.at[l], w_ref.at[l], sems.at[2 + l]))
    for copy in copies:
        copy.start()
    for copy in copies:
        copy.wait()


def load_more_kernel(start, w_hbm, w_ref, sems):
    copies = [
        pltpu.make_async_copy(w_hbm.at[start + l], w_ref.at[l], sems.at[l])
        for l in range(w_ref.shape[0])
    ]
    for copy in copies:
        copy.start()
    for copy in copies:
        copy.wait()


def store_products(l, row, col, row_keep, up_send, down_send, col_keep, col_send):
    rank = row.shape[0] // 2
    row_keep[l] = row
    up_send[l] = row[:rank].astype(BF16)
    down_send[l] = row[rank:].astype(BF16)
    col_keep[l] = col
    col_send[l] = col.astype(BF16)


def first_products_kernel(w_hbm, w_a, w_b, up_ref, down_ref, left_ref, right_ref, *refs):
    w_c, *outs, sems = refs
    early, late = w_a.shape[0] + w_b.shape[0], w_c.shape[0]
    even = is_even("col")
    copies = [
        pltpu.make_async_copy(w_hbm.at[early + l], w_c.at[l], sems.at[l]) for l in range(late)
    ]
    for copy in copies:
        copy.start()
    for l in range(early + late):
        if l >= early:
            copies[l - early].wait()
        ref, at = layer_of((w_a, w_b, w_c), l)
        left, right = left_ref[l], right_ref[l]
        cols = [jnp.where(even, right, left), jnp.where(even, left, right)]
        factors = jnp.concatenate([up_ref[l], down_ref[l]] + cols, axis=0)
        products = rows_by_features(factors, ref[at])
        half = products.shape[0] // 2
        store_products(l, products[:half], products[half:], *outs)


def middle_col_kernel(partners, col_keep, *refs):
    received, (col_total, even_send, odd_send) = refs[:partners], refs[partners:]
    rank = even_send.shape[1]
    for l in range(col_keep.shape[0]):
        col = col_keep[l]
        for other in received:
            col = col + other[l].astype(F32)
        col_total[l] = col
        even_send[l] = col[:rank].astype(BF16)
        odd_send[l] = col[rank:].astype(BF16)


def middle_row_kernel(row_keep, from_above, from_below, row_diff, row_send):
    for l in range(row_keep.shape[0]):
        row = row_keep[l] - jnp.concatenate([from_above[l], from_below[l]], axis=0).astype(F32)
        row_diff[l] = row
        row_send[l] = row.astype(BF16)


def lane_sum(parts):
    total = parts[0]
    for part in parts[1:]:
        total = total + part
    return jnp.sum(total, axis=1, keepdims=True)


def orthonormal(v_ref, rank):
    tiles, stack, _ = v_ref.shape
    groups = stack // rank

    def vector(k):
        return [v_ref[t, pl.ds(k, groups, stride=rank), :] for t in range(tiles)]

    rest = [vector(k) for k in range(rank)]
    for k in range(rank):
        u = rest[k]
        square = lane_sum([x * x for x in u]) + epsilon
        for j in range(k + 1, rank):
            along = lane_sum([x * y for x, y in zip(vector(j), u)]) / square
            rest[j] = [x - along * y for x, y in zip(rest[j], u)]
        scale = 1.0 / jnp.sqrt(square)
        rest[k] = [x * scale for x in u]
    for k in range(rank):
        for t in range(tiles):
            v_ref[t, pl.ds(k, groups, stride=rank), :] = rest[k][t]


def store_vectors(v_ref, rows, values):
    for t in range(v_ref.shape[0]):
        v_ref[t, rows, :] = values[:, 128 * t : 128 * (t + 1)]


def back_products(v_ref, w_refs, pairs, basis_ref, back_ref, sends, layers):
    tiles, stack, _ = v_ref.shape
    pair = stack // layers
    rank = pair // 2
    orthonormal(v_ref, rank)
    basis = jnp.concatenate([v_ref[t] for t in range(tiles)], axis=1)
    basis_ref[...] = basis.astype(BF16)
    changes = None
    for old_basis, old_factors in pairs:
        mixing = within_layers(rows_by_features(basis.astype(BF16), old_basis[...]), pair)
        change = small_times(mixing, old_factors[...])
        changes = change if changes is None else changes + change
    for l in range(layers):
        here = slice(l * pair, (l + 1) * pair)
        ref, at = layer_of(w_refs, l)
        back = jnp.dot(basis[here].astype(BF16), ref[at], preferred_element_type=F32)
        if changes is not None:
            back = back + changes[here]
        back_ref[here, :] = back
        for i, send in enumerate(sends):
            send[l] = back[rank * i : rank * i + rank].astype(BF16)


def back_col_kernel(earlier, w_a, w_b, w_c, col_total, from_even, from_odd, *refs):
    pairs, refs = refs[: 2 * earlier], refs[2 * earlier :]
    basis_ref, back_ref, *sends, v_ref = refs
    layers, pair, _ = col_total.shape
    for l in range(layers):
        theirs = jnp.concatenate([from_even[l], from_odd[l]], axis=0).astype(F32)
        store_vectors(v_ref, slice(l * pair, (l + 1) * pair), col_total[l] - theirs)
    pairs = list(zip(pairs[::2], pairs[1::2]))
    back_products(v_ref, (w_a, w_b, w_c), pairs, basis_ref, back_ref, sends, layers)


def back_row_kernel(partners, earlier, w_a, w_b, w_c, row_diff, *refs):
    received, refs = refs[:partners], refs[partners:]
    pairs, refs = refs[: 2 * earlier], refs[2 * earlier :]
    basis_ref, back_ref, *sends, v_ref = refs
    layers, pair, _ = row_diff.shape
    for l in range(layers):
        row = row_diff[l]
        for other in received:
            row = row + other[l].astype(F32)
        store_vectors(v_ref, slice(l * pair, (l + 1) * pair), row)
    pairs = list(zip(pairs[::2], pairs[1::2]))
    back_products(v_ref, (w_a, w_b, w_c), pairs, basis_ref, back_ref, sends, layers)


def combined_of(l, back_ref, first, second):
    pair = 2 * first.shape[1]
    theirs = jnp.concatenate([first[l], second[l]], axis=0)
    return back_ref[l * pair : (l + 1) * pair, :] + theirs.astype(F32)


def next_products_kernel(earlier, w_a, w_b, w_c, *refs):
    (row_back, col_back, above, below, at_even, at_odd), refs = refs[:6], refs[6:]
    pairs, refs = refs[: 2 * earlier], refs[2 * earlier :]
    row_basis, col_basis, bases_ref, factors_ref, *outs, f_ref = refs
    layers, rank, _ = above.shape
    pair, stack = 2 * rank, row_basis.shape[0]
    bases_ref[:stack, :] = row_basis[...]
    bases_ref[stack:, :] = col_basis[...]
    for l in range(layers):
        f_ref[l * pair : (l + 1) * pair, :] = combined_of(l, row_back, above, below)
        f_ref[stack + l * pair : stack + (l + 1) * pair, :] = combined_of(l, col_back, at_even, at_odd)
    factors = f_ref[...].astype(BF16)
    factors_ref[...] = factors
    known = list(zip(pairs[::2], pairs[1::2])) + [(bases_ref, factors_ref)]
    changes = None
    for old_basis, old_factors in known:
        mixing = within_layers(rows_by_features(factors, old_factors[...]), pair)
        change = small_times(mixing, old_basis[...])
        changes = change if changes is None else changes + change
    for l in range(layers):
        row_at = slice(l * pair, (l + 1) * pair)
        col_at = slice(stack + l * pair, stack + (l + 1) * pair)
        own = jnp.concatenate([f_ref[row_at, :], f_ref[col_at, :]], axis=0).astype(BF16)
        ref, at = layer_of((w_a, w_b, w_c), l)
        products = rows_by_features(own, ref[at])
        store_products(
            l, products[:pair] + changes[row_at], products[pair:] + changes[col_at], *outs
        )


def finish_kernel(earlier, chunk, w_a, w_b, w_c, *refs):
    (row_back, col_back, above, below, at_even, at_odd), refs = refs[:6], refs[6:]
    pairs, refs = refs[: 2 * earlier], refs[2 * earlier :]
    row_basis, col_basis, w_out, down_out, right_out, staged, sems = refs
    layers, depth, _ = staged.shape
    rank, stack = above.shape[1], row_basis.shape[0]
    pair = 2 * rank
    even = is_even("col")
    copies = []
    for l in range(layers):
        row_at = slice(l * pair, (l + 1) * pair)
        col_at = slice(stack + l * pair, stack + (l + 1) * pair)
        row = combined_of(l, row_back, above, below)
        col = combined_of(l, col_back, at_even, at_odd)
        down_out[l] = row[rank:]
        right_out[l] = jnp.where(even, col[:rank], col[rank:])
        old = [f[at, :] for f in pairs[1::2] for at in (row_at, col_at)]
        factors = jnp.concatenate(old + [row.astype(BF16), col.astype(BF16)], axis=0)
        ref, at = layer_of((w_a, w_b, w_c), l)
        for c in range(depth // chunk):
            part = slice(c * chunk, (c + 1) * chunk)
            old = [b[rows, part] for b in pairs[::2] for rows in (row_at, col_at)]
            basis = jnp.concatenate(
                old + [row_basis[row_at, part], col_basis[row_at, part]], axis=0
            )
            correction = lax.dot_general(
                basis, factors, (((0,), (0,)), ((), ())), preferred_element_type=F32
            )
            staged[l, part] = (ref[at, part].astype(F32) - step_size * correction).astype(BF16)
            copy = pltpu.make_async_copy(staged.at[l, part], w_out.at[l, part], sems.at[l, c])
            copy.start()
            copies.append(copy)
    for copy in copies:
        copy.wait()


def body(weights, warm_down, warm_right):
    vmem, hbm = pltpu.VMEM, pltpu.HBM
    w_hbm, down_hbm, right_hbm = (
        pltpu.with_memory_space_constraint(x[0, 0], hbm) for x in (weights, warm_down, warm_right)
    )
    count, depth, width = w_hbm.shape
    rank = down_hbm.shape[1]
    partners = lax.axis_size("mp") - 1
    pair, stack = 2 * rank, 2 * rank * count
    dma = pltpu.SemaphoreType.DMA

    def local(kernel, outs, args, **more):
        return call(kernel, outs, args, [vmem] * len(args), **more)

    kept = ((count, pair, depth), F32, vmem)
    both_edges = ((count, pair, depth), BF16, vmem)
    one_edge = ((count, rank, depth), BF16, vmem)
    product_outs = [kept, one_edge, one_edge, kept, both_edges]
    own_factors = ((count, rank, width), BF16, vmem)
    back_outs = [((stack, depth), BF16, vmem), ((stack, width), F32, vmem), own_factors, own_factors]
    vectors = [pltpu.VMEM((depth // 128, stack, 128), F32)]

    some, more = max(1, count // 5), max(1, 2 * count // 5)
    w_a, own_down, own_right = call(
        load_kernel,
        [((some, depth, width), BF16, vmem), own_factors, own_factors],
        (w_hbm, down_hbm, right_hbm),
        [hbm] * 3,
        scratch=[dma((some + 2,))],
    )
    above = passed_along(own_down, "row", 1)
    beside = passed_along(own_right, "col", 1)
    (w_b,) = call(
        functools.partial(load_more_kernel, some),
        [((more, depth, width), BF16, vmem)],
        (w_hbm,),
        [hbm],
        scratch=[dma((more,))],
        flops=100_000_000,
    )
    rest = count - some - more
    w_c, *products = call(
        first_products_kernel,
        [((rest, depth, width), BF16, vmem)] + product_outs,
        (w_hbm, w_a, w_b, above, own_down, beside, own_right),
        [hbm] + [vmem] * 6,
        scratch=[dma((rest,))],
    )
    w = (w_a, w_b, w_c)
    pairs = ()
    for repeat in range(ROUNDS):
        row_keep, up_send, down_send, col_keep, col_send = products
        col_received = from_partners(col_send, "mp")
        from_above = passed_along(down_send, "row", 1)
        from_below = passed_along(up_send, "row", -1)
        col_total, even_send, odd_send = local(
            functools.partial(middle_col_kernel, partners),
            [kept, one_edge, one_edge],
            (col_keep, *col_received),
        )
        from_odd = exchanged(odd_send, "col", 1)
        from_even = exchanged(even_send, "col", 0)
        row_diff, row_send = local(
            middle_row_kernel, [kept, both_edges], (row_keep, from_above, from_below)
        )
        row_received = from_partners(row_send, "mp")
        col_basis, col_back, even_send, odd_send = local(
            functools.partial(back_col_kernel, repeat),
            back_outs,
            (*w, col_total, from_even, from_odd, *pairs),
            scratch=vectors,
        )
        from_odd = exchanged(odd_send, "col", 1)
        from_even = exchanged(even_send, "col", 0)
        row_basis, row_back, up_send, down_send = local(
            functools.partial(back_row_kernel, partners, repeat),
            back_outs,
            (*w, row_diff, *row_received, *pairs),
            scratch=vectors,
        )
        from_above = passed_along(down_send, "row", 1)
        from_below = passed_along(up_send, "row", -1)
        moved = (row_back, col_back, from_above, from_below, from_even, from_odd)
        args = (*w, *moved, *pairs, row_basis, col_basis)
        if repeat + 1 < ROUNDS:
            bases, factors, *products = local(
                functools.partial(next_products_kernel, repeat),
                [((2 * stack, depth), BF16, vmem), ((2 * stack, width), BF16, vmem)] + product_outs,
                args,
                scratch=[pltpu.VMEM((2 * stack, width), F32)],
            )
            pairs = (*pairs, bases, factors)
    chunk = depth // 3 if depth % 384 == 0 else depth
    new_w, next_down, next_right = local(
        functools.partial(finish_kernel, ROUNDS - 1, chunk),
        [
            ((count, depth, width), BF16, hbm),
            ((count, rank, width), F32, vmem),
            ((count, rank, width), F32, vmem),
        ],
        args,
        scratch=[pltpu.VMEM((count, depth, width), BF16), dma((count, depth // chunk))],
        limit=28,
    )
    return new_w[None, None], next_down[None, None], next_right[None, None]


def solution(mesh):
    placed = (P("row", "col", None, None, "mp"),) * 3
    return jax.shard_map(body, mesh=mesh, in_specs=placed, out_specs=placed, check_vma=False)
```

```python
import functools

import jax
import jax.numpy as jnp
from jax import lax
from jax.experimental import pallas as pl
from jax.experimental.pallas import tpu as pltpu
from jax.sharding import PartitionSpec as P


ROUNDS = 2
step_size = 0.2
epsilon = 1e-06

BF16 = jnp.bfloat16
F32 = jnp.float32
MIB = 1024 * 1024


def passed_along(value, axis, by):
    devices = lax.axis_size(axis)
    return lax.ppermute(value, axis, [(i, (i + by) % devices) for i in range(devices)])


def exchanged(value, axis, place):
    devices = lax.axis_size(axis)
    pairs = []
    for i in range(place, devices, 2):
        pairs += [(i, (i + 1) % devices), ((i + 1) % devices, i)]
    return lax.ppermute(value, axis, sorted(pairs))


def is_even(axis):
    return lax.rem(lax.axis_index(axis), 2) == 0


def from_partners(value, axis):
    return [passed_along(value, axis, by) for by in range(1, lax.axis_size(axis))]


def call(kernel, outs, args, arg_spaces, scratch=(), limit=16, flops=1_000_000):
    return pl.pallas_call(
        kernel,
        out_shape=[jax.ShapeDtypeStruct(shape, dtype) for shape, dtype, _ in outs],
        in_specs=[pl.BlockSpec(memory_space=space) for space in arg_spaces],
        out_specs=[pl.BlockSpec(memory_space=space) for _, _, space in outs],
        scratch_shapes=list(scratch),
        compiler_params=pltpu.CompilerParams(vmem_limit_bytes=limit * MIB),
        cost_estimate=pl.CostEstimate(flops=flops, bytes_accessed=0, transcendentals=0),
    )(*args)


def rows_by_features(left, right):
    return lax.dot_general(left, right, (((1,), (1,)), ((), ())), preferred_element_type=F32)


def layer_of(w_refs, l):
    for ref in w_refs:
        if l < ref.shape[0]:
            return ref, l
        l -= ref.shape[0]


def within_layers(mixing, pair):
    rows, cols = mixing.shape
    row = lax.broadcasted_iota(jnp.int32, (rows, cols), 0)
    col = lax.broadcasted_iota(jnp.int32, (rows, cols), 1)
    stack = cols // 2
    row = jnp.where(row < stack, row, row - stack) // pair
    col = jnp.where(col < stack, col, col - stack) // pair
    return jnp.where(row == col, -step_size * mixing, 0.0)


def small_times(small, wide):
    high = small.astype(BF16)
    low = (small - high.astype(F32)).astype(BF16)
    both = jnp.dot(jnp.concatenate([high, low], axis=0), wide, preferred_element_type=F32)
    return both[: small.shape[0]] + both[small.shape[0] :]


def load_kernel(w_hbm, down_hbm, right_hbm, w_ref, down_ref, right_ref, sems):
    copies = [
        pltpu.make_async_copy(down_hbm, down_ref, sems.at[0]),
        pltpu.make_async_copy(right_hbm, right_ref, sems.at[1]),
    ]
    for l in range(w_ref.shape[0]):
        copies.append(pltpu.make_async_copy(w_hbm.at[l], w_ref.at[l], sems.at[2 + l]))
    for copy in copies:
        copy.start()
    for copy in copies:
        copy.wait()


def store_products(l, row, col, row_keep, up_send, down_send, col_keep, col_send):
    rank = row.shape[0] // 2
    row_keep[l] = row
    up_send[l] = row[:rank].astype(BF16)
    down_send[l] = row[rank:].astype(BF16)
    col_keep[l] = col
    col_send[l] = col.astype(BF16)


def first_products_kernel(w_hbm, w_a, up_ref, down_ref, left_ref, right_ref, *refs):
    w_c, *outs, sems = refs
    early, late = w_a.shape[0], w_c.shape[0]
    even = is_even("col")
    copies = [
        pltpu.make_async_copy(w_hbm.at[early + l], w_c.at[l], sems.at[l]) for l in range(late)
    ]
    for copy in copies:
        copy.start()
    for l in range(early + late):
        if l >= early:
            copies[l - early].wait()
        ref, at = layer_of((w_a, w_c), l)
        left, right = left_ref[l], right_ref[l]
        cols = [jnp.where(even, right, left), jnp.where(even, left, right)]
        factors = jnp.concatenate([up_ref[l], down_ref[l]] + cols, axis=0)
        products = rows_by_features(factors, ref[at])
        half = products.shape[0] // 2
        store_products(l, products[:half], products[half:], *outs)


def middle_col_kernel(partners, col_keep, *refs):
    received, (col_total, even_send, odd_send) = refs[:partners], refs[partners:]
    rank = even_send.shape[1]
    for l in range(col_keep.shape[0]):
        col = col_keep[l]
        for other in received:
            col = col + other[l].astype(F32)
        col_total[l] = col
        even_send[l] = col[:rank].astype(BF16)
        odd_send[l] = col[rank:].astype(BF16)


def middle_row_kernel(row_keep, from_above, from_below, row_diff, row_send):
    for l in range(row_keep.shape[0]):
        row = row_keep[l] - jnp.concatenate([from_above[l], from_below[l]], axis=0).astype(F32)
        row_diff[l] = row
        row_send[l] = row.astype(BF16)


def lane_sum(parts):
    total = parts[0]
    for part in parts[1:]:
        total = total + part
    return jnp.sum(total, axis=1, keepdims=True)


def orthonormal(v_ref, rank):
    tiles, stack, _ = v_ref.shape
    groups = stack // rank

    def vector(k):
        return [v_ref[t, pl.ds(k, groups, stride=rank), :] for t in range(tiles)]

    rest = [vector(k) for k in range(rank)]
    for k in range(rank):
        u = rest[k]
        square = lane_sum([x * x for x in u]) + epsilon
        for j in range(k + 1, rank):
            along = lane_sum([x * y for x, y in zip(vector(j), u)]) / square
            rest[j] = [x - along * y for x, y in zip(rest[j], u)]
        scale = 1.0 / jnp.sqrt(square)
        rest[k] = [x * scale for x in u]
    for k in range(rank):
        for t in range(tiles):
            v_ref[t, pl.ds(k, groups, stride=rank), :] = rest[k][t]


def store_vectors(v_ref, rows, values):
    for t in range(v_ref.shape[0]):
        v_ref[t, rows, :] = values[:, 128 * t : 128 * (t + 1)]


def back_products(v_ref, w_refs, pairs, basis_ref, back_ref, sends, layers):
    tiles, stack, _ = v_ref.shape
    pair = stack // layers
    rank = pair // 2
    orthonormal(v_ref, rank)
    basis = jnp.concatenate([v_ref[t] for t in range(tiles)], axis=1)
    basis_ref[...] = basis.astype(BF16)
    changes = None
    for old_basis, old_factors in pairs:
        mixing = within_layers(rows_by_features(basis.astype(BF16), old_basis[...]), pair)
        change = small_times(mixing, old_factors[...])
        changes = change if changes is None else changes + change
    for l in range(layers):
        here = slice(l * pair, (l + 1) * pair)
        ref, at = layer_of(w_refs, l)
        back = jnp.dot(basis[here].astype(BF16), ref[at], preferred_element_type=F32)
        if changes is not None:
            back = back + changes[here]
        back_ref[here, :] = back
        for i, send in enumerate(sends):
            send[l] = back[rank * i : rank * i + rank].astype(BF16)


def back_col_kernel(earlier, w_a, w_c, col_total, from_even, from_odd, *refs):
    pairs, refs = refs[: 2 * earlier], refs[2 * earlier :]
    basis_ref, back_ref, *sends, v_ref = refs
    layers, pair, _ = col_total.shape
    for l in range(layers):
        theirs = jnp.concatenate([from_even[l], from_odd[l]], axis=0).astype(F32)
        store_vectors(v_ref, slice(l * pair, (l + 1) * pair), col_total[l] - theirs)
    pairs = list(zip(pairs[::2], pairs[1::2]))
    back_products(v_ref, (w_a, w_c), pairs, basis_ref, back_ref, sends, layers)


def back_row_kernel(partners, earlier, w_a, w_c, row_diff, *refs):
    received, refs = refs[:partners], refs[partners:]
    pairs, refs = refs[: 2 * earlier], refs[2 * earlier :]
    basis_ref, back_ref, *sends, v_ref = refs
    layers, pair, _ = row_diff.shape
    for l in range(layers):
        row = row_diff[l]
        for other in received:
            row = row + other[l].astype(F32)
        store_vectors(v_ref, slice(l * pair, (l + 1) * pair), row)
    pairs = list(zip(pairs[::2], pairs[1::2]))
    back_products(v_ref, (w_a, w_c), pairs, basis_ref, back_ref, sends, layers)


def combined_of(l, back_ref, first, second):
    pair = 2 * first.shape[1]
    theirs = jnp.concatenate([first[l], second[l]], axis=0)
    return back_ref[l * pair : (l + 1) * pair, :] + theirs.astype(F32)


def next_products_kernel(earlier, w_a, w_c, *refs):
    (row_back, col_back, above, below, at_even, at_odd), refs = refs[:6], refs[6:]
    pairs, refs = refs[: 2 * earlier], refs[2 * earlier :]
    row_basis, col_basis, bases_ref, factors_ref, *outs, f_ref = refs
    layers, rank, _ = above.shape
    pair, stack = 2 * rank, row_basis.shape[0]
    bases_ref[:stack, :] = row_basis[...]
    bases_ref[stack:, :] = col_basis[...]
    for l in range(layers):
        f_ref[l * pair : (l + 1) * pair, :] = combined_of(l, row_back, above, below)
        f_ref[stack + l * pair : stack + (l + 1) * pair, :] = combined_of(l, col_back, at_even, at_odd)
    factors = f_ref[...].astype(BF16)
    factors_ref[...] = factors
    known = list(zip(pairs[::2], pairs[1::2])) + [(bases_ref, factors_ref)]
    changes = None
    for old_basis, old_factors in known:
        mixing = within_layers(rows_by_features(factors, old_factors[...]), pair)
        change = small_times(mixing, old_basis[...])
        changes = change if changes is None else changes + change
    for l in range(layers):
        row_at = slice(l * pair, (l + 1) * pair)
        col_at = slice(stack + l * pair, stack + (l + 1) * pair)
        own = jnp.concatenate([f_ref[row_at, :], f_ref[col_at, :]], axis=0).astype(BF16)
        ref, at = layer_of((w_a, w_c), l)
        products = rows_by_features(own, ref[at])
        store_products(
            l, products[:pair] + changes[row_at], products[pair:] + changes[col_at], *outs
        )


def finish_kernel(earlier, chunk, w_a, w_c, *refs):
    (row_back, col_back, above, below, at_even, at_odd), refs = refs[:6], refs[6:]
    pairs, refs = refs[: 2 * earlier], refs[2 * earlier :]
    row_basis, col_basis, w_out, down_out, right_out, staged, sems = refs
    layers, depth, _ = staged.shape
    rank, stack = above.shape[1], row_basis.shape[0]
    pair = 2 * rank
    even = is_even("col")
    copies = []
    for l in range(layers):
        row_at = slice(l * pair, (l + 1) * pair)
        col_at = slice(stack + l * pair, stack + (l + 1) * pair)
        row = combined_of(l, row_back, above, below)
        col = combined_of(l, col_back, at_even, at_odd)
        down_out[l] = row[rank:]
        right_out[l] = jnp.where(even, col[:rank], col[rank:])
        old = [f[at, :] for f in pairs[1::2] for at in (row_at, col_at)]
        factors = jnp.concatenate(old + [row.astype(BF16), col.astype(BF16)], axis=0)
        ref, at = layer_of((w_a, w_c), l)
        for c in range(depth // chunk):
            part = slice(c * chunk, (c + 1) * chunk)
            old = [b[rows, part] for b in pairs[::2] for rows in (row_at, col_at)]
            basis = jnp.concatenate(
                old + [row_basis[row_at, part], col_basis[row_at, part]], axis=0
            )
            correction = lax.dot_general(
                basis, factors, (((0,), (0,)), ((), ())), preferred_element_type=F32
            )
            staged[l, part] = (ref[at, part].astype(F32) - step_size * correction).astype(BF16)
            copy = pltpu.make_async_copy(staged.at[l, part], w_out.at[l, part], sems.at[l, c])
            copy.start()
            copies.append(copy)
    for copy in copies:
        copy.wait()


def body(weights, warm_down, warm_right):
    vmem, hbm = pltpu.VMEM, pltpu.HBM
    w_hbm, down_hbm, right_hbm = (
        pltpu.with_memory_space_constraint(x[0, 0], hbm) for x in (weights, warm_down, warm_right)
    )
    count, depth, width = w_hbm.shape
    rank = down_hbm.shape[1]
    partners = lax.axis_size("mp") - 1
    pair, stack = 2 * rank, 2 * rank * count
    dma = pltpu.SemaphoreType.DMA

    def local(kernel, outs, args, **more):
        return call(kernel, outs, args, [vmem] * len(args), **more)

    kept = ((count, pair, depth), F32, vmem)
    both_edges = ((count, pair, depth), BF16, vmem)
    one_edge = ((count, rank, depth), BF16, vmem)
    product_outs = [kept, one_edge, one_edge, kept, both_edges]
    own_factors = ((count, rank, width), BF16, vmem)
    back_outs = [((stack, depth), BF16, vmem), ((stack, width), F32, vmem), own_factors, own_factors]
    vectors = [pltpu.VMEM((depth // 128, stack, 128), F32)]

    some = max(1, 3 * count // 5)
    above = passed_along(warm_down[0, 0], "row", 1)
    beside = passed_along(warm_right[0, 0], "col", 1)
    w_a, own_down, own_right = call(
        load_kernel,
        [((some, depth, width), BF16, vmem), own_factors, own_factors],
        (w_hbm, down_hbm, right_hbm),
        [hbm] * 3,
        scratch=[dma((some + 2,))],
        flops=100_000_000,
    )
    rest = count - some
    w_c, *products = call(
        first_products_kernel,
        [((rest, depth, width), BF16, vmem)] + product_outs,
        (w_hbm, w_a, above, own_down, beside, own_right),
        [hbm] + [vmem] * 5,
        scratch=[dma((rest,))],
    )
    w = (w_a, w_c)
    pairs = ()
    for repeat in range(ROUNDS):
        row_keep, up_send, down_send, col_keep, col_send = products
        col_received = from_partners(col_send, "mp")
        from_above = passed_along(down_send, "row", 1)
        from_below = passed_along(up_send, "row", -1)
        col_total, even_send, odd_send = local(
            functools.partial(middle_col_kernel, partners),
            [kept, one_edge, one_edge],
            (col_keep, *col_received),
        )
        from_odd = exchanged(odd_send, "col", 1)
        from_even = exchanged(even_send, "col", 0)
        row_diff, row_send = local(
            middle_row_kernel, [kept, both_edges], (row_keep, from_above, from_below)
        )
        row_received = from_partners(row_send, "mp")
        col_basis, col_back, even_send, odd_send = local(
            functools.partial(back_col_kernel, repeat),
            back_outs,
            (*w, col_total, from_even, from_odd, *pairs),
            scratch=vectors,
        )
        from_odd = exchanged(odd_send, "col", 1)
        from_even = exchanged(even_send, "col", 0)
        row_basis, row_back, up_send, down_send = local(
            functools.partial(back_row_kernel, partners, repeat),
            back_outs,
            (*w, row_diff, *row_received, *pairs),
            scratch=vectors,
        )
        from_above = passed_along(down_send, "row", 1)
        from_below = passed_along(up_send, "row", -1)
        moved = (row_back, col_back, from_above, from_below, from_even, from_odd)
        args = (*w, *moved, *pairs, row_basis, col_basis)
        if repeat + 1 < ROUNDS:
            bases, factors, *products = local(
                functools.partial(next_products_kernel, repeat),
                [((2 * stack, depth), BF16, vmem), ((2 * stack, width), BF16, vmem)] + product_outs,
                args,
                scratch=[pltpu.VMEM((2 * stack, width), F32)],
            )
            pairs = (*pairs, bases, factors)
    chunk = depth // 6 if depth % 768 == 0 else depth
    new_w, next_down, next_right = local(
        functools.partial(finish_kernel, ROUNDS - 1, chunk),
        [
            ((count, depth, width), BF16, hbm),
            ((count, rank, width), F32, vmem),
            ((count, rank, width), F32, vmem),
        ],
        args,
        scratch=[pltpu.VMEM((count, depth, width), BF16), dma((count, depth // chunk))],
        limit=28,
    )
    return new_w[None, None], next_down[None, None], next_right[None, None]


def solution(mesh):
    placed = (P("row", "col", None, None, "mp"),) * 3
    return jax.shard_map(body, mesh=mesh, in_specs=placed, out_specs=placed, check_vma=False)
```
